32 devices in a mesh: krow: 16 (over z, x, core), kcol: 2 (over y).
Axes of the slice: x: 2, y: 2, z: 4, core: 2. Of those that a mesh axis runs over, the one named last changes fastest.
Arguments:
- green: bfloat16 [4, 2, 16, 4, 256, 256], P(None, None, 'krow', 'kcol'), may hold values from -6 to 6
- screened: float32 [16, 4, 65536], P(None, None, ('krow', 'kcol')), may hold values from 0.1 to 1
Outputs:
- sigma: bfloat16 [4, 2, 16, 4, 256, 256], P(None, None, 'krow', 'kcol')
- dressed: bfloat16 [4, 2, 16, 4, 256, 256], P(None, None, 'krow', 'kcol')
The draws below stay inside these ranges and needn't reach their ends.
All inputs are finite; a program needn't handle non-finite values.
Results may differ from the reference program's by a relative error of at most 0.0053.
Values may be sent and summed in bfloat16 or wider, within the bound.
No kernel may reach another device: no remote copies, remote signals or barrier semaphores. Data moves between devices by JAX's collectives and lax.ppermute only.
A program may use at most 64 MiB of HBM per device.

```python
import math
import jax
import jax.numpy as jnp
from jax import lax

NO = 256
NE = 4
K1 = 16
K2 = 4
PAIRS = 65536


def block_levels(own_key, dims, cuts, low, largest):
    def one(position, parts):
        draws = jax.random.uniform(jax.random.fold_in(jax.random.fold_in(own_key, 6), position), (parts,), jnp.float32, low / len(cuts), largest / len(cuts))
        return jnp.repeat(jnp.exp(draws), dims[position] // parts).reshape((-1,) + (1,) * (len(dims) - position - 1))

    factor_of = one(*cuts[0])
    for cut in cuts[1:]:
        factor_of = factor_of * one(*cut)
    return factor_of


def noise(stream_key, shape, scale, reach, pieces=(), kind=jnp.bfloat16):
    level = block_levels(stream_key, shape, pieces, -0.22, 0.18) if pieces else 1.0
    array = jax.random.normal(stream_key, shape, jnp.float32) * scale * level
    return jnp.minimum(jnp.maximum(array, -reach), reach).astype(kind)


def setup_inputs(seed: int = 0) -> dict:
    key_of = jax.random.split(jax.random.key(seed), 3)
    return {
        "green": noise(key_of[0], (NE, 2, K1, K2, NO, NO), 1.0, 6.0, ((2, 16), (3, 2))),
        "screened": jnp.clip(0.1 + 0.9 * jax.random.uniform(key_of[1], (K1, K2, PAIRS), jnp.float32) ** block_levels(key_of[1], (K1, K2, PAIRS), ((2, 32),), -0.2, 0.2), 0.1, 1.0),
    }


full_turn = 2.0 * math.pi


def phase_tables(length, forward):
    step_counter = jnp.arange(length, dtype=jnp.int32)
    product = (step_counter[:, None] * step_counter[None, :]) % length
    angles = full_turn * product.astype(jnp.float32) / length
    if forward:
        return jnp.cos(angles) / length, jnp.sin(angles) / length
    return jnp.cos(angles), -jnp.sin(angles)


def apply_over_axis(matrix, values, along_dim):
    letters = "abcdefgh"[:values.ndim]
    target = letters[:along_dim] + "z" + letters[along_dim + 1:]
    formula = "z" + letters[along_dim] + "," + letters + "->" + target
    return jnp.einsum(formula, matrix, values, precision=lax.Precision.HIGHEST)


def complex_along(state, cosine, sine, along_dim):
    real_part, imag_part = state
    out_real = apply_over_axis(cosine, real_part, along_dim) - apply_over_axis(sine, imag_part, along_dim)
    out_imag = apply_over_axis(sine, real_part, along_dim) + apply_over_axis(cosine, imag_part, along_dim)
    return out_real, out_imag


def matmul_batch(left, right):
    return jnp.einsum('xyij,xyjl->xyil', left, right, precision=lax.Precision.HIGHEST)


def reference(green, screened):
    fwd_one = phase_tables(K1, True)
    fwd_two = phase_tables(K2, True)
    inv_one = phase_tables(K1, False)
    inv_two = phase_tables(K2, False)
    pair_weights = screened.reshape(K1, K2, NO, NO)
    green_rows = jnp.moveaxis(green, 4, 0)
    weight_rows = jnp.moveaxis(pair_weights, 2, 0)

    def one_row(operand_list):
        block, wblock = operand_list
        state = (block[:, 0].astype(jnp.float32), block[:, 1].astype(jnp.float32))
        state = complex_along(state, fwd_one[0], fwd_one[1], 1)
        state = complex_along(state, fwd_two[0], fwd_two[1], 2)
        state = (-wblock * state[0], -wblock * state[1])
        state = complex_along(state, inv_one[0], inv_one[1], 1)
        state = complex_along(state, inv_two[0], inv_two[1], 2)
        return jnp.stack(state, 1).astype(jnp.bfloat16)

    sigma = lax.map(one_row, (green_rows, weight_rows))
    sigma = jnp.moveaxis(sigma, 0, 4)

    def one_energy(operand_list):
        green_value_list, self_energy_values = operand_list
        green_real = green_value_list[0].astype(jnp.float32)
        green_imag = green_value_list[1].astype(jnp.float32)
        self_energy_real = self_energy_values[0].astype(jnp.float32)
        self_energy_imaginary = self_energy_values[1].astype(jnp.float32)
        kern_real = matmul_batch(green_real, self_energy_real) - matmul_batch(green_imag, self_energy_imaginary)
        kern_imag = matmul_batch(green_real, self_energy_imaginary) + matmul_batch(green_imag, self_energy_real)
        kern_real = lax.optimization_barrier(kern_real.astype(jnp.bfloat16)).astype(jnp.float32)
        kern_imag = lax.optimization_barrier(kern_imag.astype(jnp.bfloat16)).astype(jnp.float32)
        corr_real = matmul_batch(kern_real, green_real) - matmul_batch(kern_imag, green_imag)
        corr_imag = matmul_batch(kern_real, green_imag) + matmul_batch(kern_imag, green_real)
        return jnp.stack((green_real + corr_real / NO, green_imag + corr_imag / NO), 0).astype(jnp.bfloat16)

    dressed = lax.map(one_energy, (green, sigma))
    return sigma, dressed
```

```python
import math

import jax
import jax.numpy as jnp
import numpy as np
from jax import lax
from jax.experimental import pallas as pl
from jax.experimental.pallas import tpu as pltpu
from jax.sharding import PartitionSpec as P

AXES = ("krow", "kcol")
ENERGY_CHUNKS = 1


def phase(length, sign):
    step = np.arange(length)
    angle = 2.0 * math.pi * (step[:, None] * step[None, :] % length) / length
    return np.cos(angle), sign * np.sin(angle)


def split_high_low(table):
    high = jnp.asarray(table, jnp.float32).astype(jnp.bfloat16)
    rest = jnp.asarray(table, jnp.float32) - high.astype(jnp.float32)
    return jnp.concatenate((high, rest.astype(jnp.bfloat16)), 0)


def row_tables(k_one, k_two, rows):
    tables = []
    for sign, scale in ((1.0, -1.0 / (k_one * k_two)), (-1.0, 1.0)):
        cosine, sine = phase(k_one, sign)
        block = np.empty((k_one, 2, k_one, 2))
        block[:, 0, :, 0] = cosine
        block[:, 0, :, 1] = -sine
        block[:, 1, :, 0] = sine
        block[:, 1, :, 1] = cosine
        square = block.reshape(2 * k_one, 2 * k_one) * scale
        tables.append(split_high_low(np.kron(square, np.eye(rows))))
    return tables


def turned(value, part, length, sign):
    re, im = value
    if part == 0:
        return value
    if 4 * part == length:
        return (-im, re) if sign > 0 else (im, -re)
    cosine = math.cos(2.0 * math.pi * part / length)
    sine = sign * math.sin(2.0 * math.pi * part / length)
    return cosine * re - sine * im, sine * re + cosine * im


def turns(values, sign):
    length = len(values)
    if length == 1:
        return values
    if length % 2:
        sums = []
        for r in range(length):
            terms = [turned(v, k * r % length, length, sign) for k, v in enumerate(values)]
            sums.append((sum(t[0] for t in terms), sum(t[1] for t in terms)))
        return sums
    even, odd = turns(values[::2], sign), turns(values[1::2], sign)
    odd = [turned(v, r, length, sign) for r, v in enumerate(odd)]
    pairs = list(zip(even, odd))
    return [(a[0] + b[0], a[1] + b[1]) for a, b in pairs] + [
        (a[0] - b[0], a[1] - b[1]) for a, b in pairs
    ]


def fourier_kernel(x_ref, w_ref, fwd_ref, inv_ref, o_ref):
    k_one, kcols, _, _, kcol_each, rows, width = x_ref.shape
    size = k_one * 2 * rows
    forward, inverse = fwd_ref[...], inv_ref[...]
    spots = [(c, k) for c in range(kcols) for k in range(kcol_each)]
    state = []
    for c, k in spots:
        block = x_ref[:, c, 0, :, k].reshape(size, width)
        both = jnp.dot(forward, block, preferred_element_type=jnp.float32)
        both = (both[:size] + both[size:]).reshape(k_one, 2, rows, width)
        state.append((both[:, 0], both[:, 1]))
    state = turns(state, 1)
    state = [(w_ref[:, r] * re, w_ref[:, r] * im) for r, (re, im) in enumerate(state)]
    state = turns(state, -1)
    for (c, k), (re, im) in zip(spots, state):
        block = jnp.stack((re, im), 1).reshape(size, width)
        high = block.astype(jnp.bfloat16)
        low = (block - high.astype(jnp.float32)).astype(jnp.bfloat16)
        both = jnp.dot(inverse, high, preferred_element_type=jnp.float32)
        out = both[:size] + both[size:]
        out = out + jnp.dot(inverse[:size], low, preferred_element_type=jnp.float32)
        o_ref[:, c, 0, :, k] = out.astype(jnp.bfloat16).reshape(k_one, 2, rows, width)


def fourier(pieces, weights, kcols):
    devices, energies, parts, each, rows, width = pieces.shape
    k_one, k_two = weights.shape[:2]
    x = pieces.reshape(k_one, kcols, energies, parts, each, rows, width)
    forward, inverse = row_tables(k_one, k_two, rows)
    block = pl.BlockSpec(
        (k_one, kcols, 1, parts, each, rows, width), lambda e: (0, 0, e, 0, 0, 0, 0)
    )
    whole = lambda a: pl.BlockSpec(a.shape, lambda e: (0,) * a.ndim)
    size = k_one * parts * rows
    out = pl.pallas_call(
        fourier_kernel,
        grid=(energies,),
        in_specs=[block, whole(weights), whole(forward), whole(inverse)],
        out_specs=block,
        out_shape=jax.ShapeDtypeStruct(x.shape, jnp.bfloat16),
        cost_estimate=pl.CostEstimate(
            flops=2 * 5 * size * size * width * k_two * energies,
            bytes_accessed=4 * x.size + 4 * weights.size,
            transcendentals=0,
        ),
        compiler_params=pltpu.CompilerParams(vmem_limit_bytes=40 * 2**20),
        name="fourier",
    )(x, weights, forward, inverse)
    return out.reshape(pieces.shape)


def dyson_kernel(s_ref, g_ref, so_ref, d_ref):
    orbitals = g_ref.shape[-1]
    sr = s_ref[:, 0, 0, 0].reshape(orbitals, orbitals)
    si = s_ref[:, 0, 1, 0].reshape(orbitals, orbitals)
    so_ref[0, 0, 0, 0] = sr
    so_ref[0, 1, 0, 0] = si
    gr, gi = g_ref[0, 0, 0, 0], g_ref[0, 1, 0, 0]
    dot = lambda a, b: jnp.dot(a, b, preferred_element_type=jnp.float32)
    kr = (dot(gr, sr) - dot(gi, si)).astype(jnp.bfloat16)
    ki = (dot(gr, si) + dot(gi, sr)).astype(jnp.bfloat16)
    scale = 1.0 / orbitals
    dr = gr.astype(jnp.float32) + (dot(kr, gr) - dot(ki, gi)) * scale
    di = gi.astype(jnp.float32) + (dot(kr, gi) + dot(ki, gr)) * scale
    d_ref[0, 0, 0, 0] = dr.astype(jnp.bfloat16)
    d_ref[0, 1, 0, 0] = di.astype(jnp.bfloat16)


def dyson(pieces, green):
    devices, energies, parts, each, rows, orbitals = pieces.shape
    flat = pl.BlockSpec(
        (1, parts, 1, 1, orbitals, orbitals), lambda e, k: (e, 0, 0, k, 0, 0)
    )
    shape = jax.ShapeDtypeStruct(green.shape, jnp.bfloat16)
    return pl.pallas_call(
        dyson_kernel,
        grid=(energies, each),
        in_specs=[
            pl.BlockSpec(
                (devices, 1, parts, 1, rows, orbitals), lambda e, k: (0, e, 0, k, 0, 0)
            ),
            flat,
        ],
        out_specs=[flat, flat],
        out_shape=[shape, shape],
        cost_estimate=pl.CostEstimate(
            flops=16 * orbitals**3 * each * energies,
            bytes_accessed=8 * green.size,
            transcendentals=0,
        ),
        name="dyson",
    )(pieces, green)


def exchange(blocks):
    return lax.all_to_all(blocks, AXES, split_axis=0, concat_axis=0, tiled=True)


def per_device(green, screened):
    kcols = lax.axis_size("kcol")
    devices = lax.axis_size("krow") * kcols
    energies, parts, _, each, orbitals, width = green.shape
    rows = orbitals // devices
    weights = screened.reshape(screened.shape[:2] + (rows, width))
    step = energies // ENERGY_CHUNKS
    chunks = [green[e : e + step] for e in range(0, energies, step)]
    middle = []
    for part in chunks:
        blocks = part.reshape(step, parts, each, devices, rows, width)
        blocks = jnp.transpose(blocks, (3, 0, 1, 2, 4, 5))
        middle.append(fourier(exchange(blocks), weights, kcols))
    outs = [dyson(exchange(m), part) for m, part in zip(middle, chunks)]
    return tuple(jnp.concatenate(o, 0) for o in zip(*outs))


def solution(mesh):
    spec = P(None, None, "krow", "kcol", None, None)
    return jax.shard_map(
        per_device,
        mesh=mesh,
        in_specs=(spec, P(None, None, AXES)),
        out_specs=(spec, spec),
        check_vma=False,
    )
```

```python
import functools
import math
import typing

import jax
import jax.numpy as jnp
import numpy as np
from jax import lax
from jax.experimental import pallas as pl
from jax.experimental.pallas import tpu as pltpu
from jax.sharding import PartitionSpec as P


AXES = ("krow", "kcol")


def phase(length, sign):
    step = np.arange(length)
    angle = 2.0 * math.pi * (step[:, None] * step[None, :] % length) / length
    return np.cos(angle), sign * np.sin(angle)


def split_high_low(table):
    high = jnp.asarray(table, jnp.float32).astype(jnp.bfloat16)
    rest = jnp.asarray(table, jnp.float32) - high.astype(jnp.float32)
    return high, rest.astype(jnp.bfloat16)


def row_tables(k_one, k_two, rows):
    tables = []
    for sign, scale in ((1.0, -1.0 / (k_one * k_two)), (-1.0, 1.0)):
        cosine, sine = phase(k_one, sign)
        block = np.empty((k_one, 2, k_one, 2))
        block[:, 0, :, 0] = cosine
        block[:, 0, :, 1] = -sine
        block[:, 1, :, 0] = sine
        block[:, 1, :, 1] = cosine
        square = block.reshape(2 * k_one, 2 * k_one) * scale
        high, low = split_high_low(np.kron(square, np.eye(rows)))
        tables.append(jnp.concatenate((high, low) if sign > 0 else (high, low, high), 1))
    return tables


def turned(value, part, length, sign):
    re, im = value
    if part == 0:
        return value
    if 4 * part == length:
        return (-im, re) if sign > 0 else (im, -re)
    cosine = math.cos(2.0 * math.pi * part / length)
    sine = sign * math.sin(2.0 * math.pi * part / length)
    return cosine * re - sine * im, sine * re + cosine * im


def turns(values, sign):
    length = len(values)
    if length == 1:
        return values
    if length % 2:
        sums = []
        for r in range(length):
            terms = [turned(v, k * r % length, length, sign) for k, v in enumerate(values)]
            sums.append((sum(t[0] for t in terms), sum(t[1] for t in terms)))
        return sums
    even, odd = turns(values[::2], sign), turns(values[1::2], sign)
    odd = [turned(v, r, length, sign) for r, v in enumerate(odd)]
    pairs = list(zip(even, odd))
    return [(a[0] + b[0], a[1] + b[1]) for a, b in pairs] + [
        (a[0] - b[0], a[1] - b[1]) for a, b in pairs
    ]


def own_index(kcols):
    return lax.axis_index("krow") * kcols + lax.axis_index("kcol")


def fourier_kernel(kcols, relative, x_ref, w_ref, fwd_ref, inv_ref, o_ref):
    devices, _, _, kcol_each, rows, width = x_ref.shape
    k_one = devices // kcols
    size = k_one * 2 * rows
    me = own_index(kcols) if relative else 0
    spots = [(c, k) for c in range(kcols) for k in range(kcol_each)]

    def slot(one, c):
        place = one * kcols + c
        return place ^ me if relative else place

    def load(c, e, k):
        parts = [x_ref[slot(one, c), e, :, k] for one in range(k_one)]
        return jnp.stack(parts, 0).reshape(size, width)

    def store(c, k, value):
        for one in range(k_one):
            o_ref[slot(one, c), 0, :, k] = value[one]

    e = pl.program_id(0)
    forward, inverse = fwd_ref[...], inv_ref[...]
    state = []
    for c, k in spots:
        block = load(c, e, k)
        block = jnp.concatenate((block, block), 0)
        out = jnp.dot(forward, block, preferred_element_type=jnp.float32)
        out = out.reshape(k_one, 2, rows, width)
        state.append((out[:, 0], out[:, 1]))
    state = turns(state, 1)
    state = [(w_ref[:, r] * re, w_ref[:, r] * im) for r, (re, im) in enumerate(state)]
    state = turns(state, -1)
    for (c, k), (re, im) in zip(spots, state):
        block = jnp.stack((re, im), 1).reshape(size, width)
        high = block.astype(jnp.bfloat16)
        low = (block - high.astype(jnp.float32)).astype(jnp.bfloat16)
        block = jnp.concatenate((high, high, low), 0)
        out = jnp.dot(inverse, block, preferred_element_type=jnp.float32)
        store(c, k, out.astype(jnp.bfloat16).reshape(k_one, 2, rows, width))


LOCAL = pl.BlockSpec(memory_space=pltpu.VMEM)


PARAMS = pltpu.CompilerParams(vmem_limit_bytes=16 * 2**20)


def near(value):
    return pltpu.with_memory_space_constraint(value, pltpu.VMEM)


def far(value):
    return pltpu.with_memory_space_constraint(value, pltpu.HBM)


def fourier(pieces, weights, kcols, relative):
    _, energies, parts, each, rows, width = pieces.shape
    k_one, k_two = weights.shape[:2]
    forward, inverse = row_tables(k_one, k_two, rows)
    size = k_one * parts * rows
    return pl.pallas_call(
        functools.partial(fourier_kernel, kcols, relative),
        grid=(energies,),
        in_specs=[LOCAL] * 4,
        out_specs=pl.BlockSpec(
            (pieces.shape[0], 1, parts, each, rows, width), lambda e: (0, e, 0, 0, 0, 0)
        ),
        out_shape=(pltpu.VMEM if relative else pltpu.HBM)(pieces.shape, jnp.bfloat16),
        cost_estimate=pl.CostEstimate(
            flops=2 * 5 * size * size * width * k_two * energies,
            bytes_accessed=4 * pieces.size + 4 * weights.size,
            transcendentals=0,
        ),
        compiler_params=PARAMS,
    )(near(pieces), near(weights), near(forward), near(inverse))


def gather_kernel(g_ref, o_ref, held, sems, out_sems):
    _, energies, parts, each = held.shape[:4]
    spots = [(p, k) for p in range(parts) for k in range(each)]
    inward = [
        [
            pltpu.make_async_copy(
                g_ref.at[e, p, k], held.at[:, e, p, k], sems.at[e, n]
            )
            for n, (p, k) in enumerate(spots)
        ]
        for e in range(energies)
    ]
    outward = [
        pltpu.make_async_copy(held.at[:, e], o_ref.at[:, e], out_sems.at[e])
        for e in range(energies)
    ]
    for copies in inward:
        for copy in copies:
            copy.start()
    for copies, last in zip(inward, outward):
        for copy in copies:
            copy.wait()
        last.start()
    for last in outward:
        last.wait()


def by_device(blocks, energies):
    _, parts, each, devices, rows, width = blocks.shape
    shape = (devices, energies, parts, each, rows, width)
    return pl.pallas_call(
        gather_kernel,
        in_specs=[pl.BlockSpec(memory_space=pltpu.HBM)],
        out_specs=pl.BlockSpec(memory_space=pltpu.HBM),
        out_shape=pltpu.HBM(shape, blocks.dtype),
        scratch_shapes=[
            pltpu.VMEM(shape, blocks.dtype),
            pltpu.SemaphoreType.DMA((energies, parts * each)),
            pltpu.SemaphoreType.DMA((energies,)),
        ],
        compiler_params=PARAMS,
        name="by_device",
    )(far(blocks))


def offset_kernel(first, kcols, g_ref, *refs):
    held, sems = refs[-2:]
    outs = refs[:-2]
    energies, parts, each, devices = held.shape[:4]
    spots = [(e, p, k) for e in range(energies) for p in range(parts) for k in range(each)]
    copies = [
        pltpu.make_async_copy(g_ref.at[first + e, p, k], held.at[e, p, k], sems.at[n])
        for n, (e, p, k) in enumerate(spots)
    ]
    for copy in copies:
        copy.start()
    me = own_index(kcols)
    share = devices // len(outs)
    for copy, (e, p, k) in zip(copies, spots):
        copy.wait()
        for j in range(devices):
            outs[j // share][j % share, e, p, k] = held[e, p, k, j ^ me]


def by_offset(blocks, first, energies, kcols, pieces):
    _, parts, each, devices, rows, width = blocks.shape
    shape = (devices // pieces, energies, parts, each, rows, width)
    return pl.pallas_call(
        functools.partial(offset_kernel, first, kcols),
        in_specs=[pl.BlockSpec(memory_space=pltpu.HBM)],
        out_specs=[LOCAL] * pieces,
        out_shape=[pltpu.VMEM(shape, blocks.dtype)] * pieces,
        scratch_shapes=[
            pltpu.VMEM((energies,) + blocks.shape[1:], blocks.dtype),
            pltpu.SemaphoreType.DMA((energies * parts * each,)),
        ],
        compiler_params=PARAMS,
        name="by_offset",
    )(far(blocks))


def dyson_kernel(first, kcols, relative, s_ref, g_ref, *refs):
    so_ref, d_ref = refs[-2:]
    devices, orbitals = s_ref.shape[0], g_ref.shape[-1]
    e, k = pl.program_id(0), pl.program_id(1)
    if relative:
        me = own_index(kcols)
        load = lambda p: jnp.stack([s_ref[d ^ me, e, p, k] for d in range(devices)], 0)
    else:
        load = lambda p: s_ref[:, e, p, k]
    sr, si = (load(p).reshape(orbitals, orbitals) for p in range(2))
    so_ref[0, 0, 0, 0] = sr
    so_ref[0, 1, 0, 0] = si
    gr, gi = g_ref[first + e, 0, 0, k], g_ref[first + e, 1, 0, k]

    def product(ar, ai, br, bi):
        left = jnp.concatenate(
            (jnp.concatenate((ar, -ai), 1), jnp.concatenate((ai, ar), 1)), 0
        )
        right = jnp.concatenate((br, bi), 0)
        out = jnp.dot(left, right, preferred_element_type=jnp.float32)
        return out[:orbitals], out[orbitals:]

    kr, ki = (a.astype(jnp.bfloat16) for a in product(gr, gi, sr, si))
    cr, ci = product(kr, ki, gr, gi)
    scale = 1.0 / orbitals
    dr = gr.astype(jnp.float32) + cr * scale
    di = gi.astype(jnp.float32) + ci * scale
    d_ref[0, 0, 0, 0] = dr.astype(jnp.bfloat16)
    d_ref[0, 1, 0, 0] = di.astype(jnp.bfloat16)


def dyson(pieces, green, first, kcols, relative, earlier):
    _, energies, parts, each, _, orbitals = pieces.shape
    flat = pl.BlockSpec(
        (1, parts, 1, 1, orbitals, orbitals), lambda e, k: (first + e, 0, 0, k, 0, 0)
    )
    shape = pltpu.HBM(green.shape, jnp.bfloat16)
    return pl.pallas_call(
        functools.partial(dyson_kernel, first, kcols, relative),
        grid=(energies, each),
        in_specs=[LOCAL, LOCAL] + [pl.BlockSpec(memory_space=pltpu.HBM)] * len(earlier),
        out_specs=[flat, flat],
        out_shape=[shape, shape],
        input_output_aliases={2 + n: n for n in range(len(earlier))},
        cost_estimate=pl.CostEstimate(
            flops=16 * orbitals**3 * each * energies,
            bytes_accessed=16 * pieces.size,
            transcendentals=0,
        ),
        compiler_params=PARAMS,
    )(near(pieces), near(green), *earlier)


def exchange(blocks):
    return lax.all_to_all(blocks, AXES, split_axis=0, concat_axis=0, tiled=True)


def swap(pieces, dims):
    counts, devices = pieces.counts, math.prod(pieces.counts)
    strides = [math.prod(counts[d + 1 :]) for d in range(len(counts))]

    def level(part, left, offset):
        if not left:
            if offset == 0:
                return part
            pairs = [(d, d ^ offset) for d in range(devices)]
            return lax.ppermute(part, AXES, pairs)
        dim, rest = left[0], left[1:]
        cut = (
            part
            if isinstance(part, (list, tuple))
            else [lax.slice_in_dim(part, q, q + 1, axis=dim) for q in range(counts[dim])]
        )
        back = [level(c, rest, offset + q * strides[dim]) for q, c in enumerate(cut)]
        return lax.concatenate(back, dim)

    return Side(counts, level(pieces.blocks, dims, 0))


class Side(typing.NamedTuple):
    counts: tuple
    blocks: typing.Any

    def merged(self):
        return self.blocks.reshape((-1,) + self.blocks.shape[len(self.counts) :])

    @classmethod
    def of(cls, counts, blocks):
        return cls(counts, blocks.reshape(counts + blocks.shape[1:]))


def per_device(green, screened):
    krows, kcols = lax.axis_size("krow"), lax.axis_size("kcol")
    devices = krows * kcols
    energies, parts, _, each, orbitals, width = green.shape
    rows = orbitals // devices
    weights = screened.reshape(screened.shape[:2] + (rows, width))
    blocks = green.reshape(energies, parts, each, devices, rows, width)
    aside = 1 if kcols == 2 and krows in (8, 16) and energies > 1 else 0
    main = energies - aside
    earlier = ()
    if aside:
        counts = (krows // 4, 2, 2, kcols)
        cut = by_offset(blocks, main, aside, kcols, counts[0])
        side = Side(counts, [c.reshape((1,) + counts[1:] + c.shape[1:]) for c in cut])
        side = swap(side, (0,))
        side = swap(side, (2,))
        side = swap(side, (1, 3))
        turned = fourier(side.merged(), weights, kcols, True)
        side = swap(Side.of(counts, turned), (2,))
        side = swap(side, (0,))
        side = swap(side, (1, 3))
        earlier = dyson(side.merged(), green, main, kcols, True, ())
    middle = exchange(by_device(blocks, main))
    middle = fourier(middle, weights, kcols, False)
    middle = exchange(middle)
    return tuple(dyson(middle, green, 0, kcols, False, earlier))


def solution(mesh):
    spec = P(None, None, "krow", "kcol", None, None)
    return jax.shard_map(
        per_device,
        mesh=mesh,
        in_specs=(spec, P(None, None, AXES)),
        out_specs=(spec, spec),
        check_vma=False,
    )
```

```python
import functools
import math
import typing

import jax
import jax.numpy as jnp
import numpy as np
from jax import lax
from jax.experimental import pallas as pl
from jax.experimental.pallas import tpu as pltpu
from jax.sharding import PartitionSpec as P


AXES = ("krow", "kcol")


def phase(length, sign):
    step = np.arange(length)
    angle = 2.0 * math.pi * (step[:, None] * step[None, :] % length) / length
    return np.cos(angle), sign * np.sin(angle)


def split_high_low(table):
    high = jnp.asarray(table, jnp.float32).astype(jnp.bfloat16)
    rest = jnp.asarray(table, jnp.float32) - high.astype(jnp.float32)
    return high, rest.astype(jnp.bfloat16)


def row_tables(k_one, k_two, rows):
    tables = []
    for sign, scale in ((1.0, -1.0 / (k_one * k_two)), (-1.0, 1.0)):
        cosine, sine = phase(k_one, sign)
        block = np.empty((k_one, 2, k_one, 2))
        block[:, 0, :, 0] = cosine
        block[:, 0, :, 1] = -sine
        block[:, 1, :, 0] = sine
        block[:, 1, :, 1] = cosine
        square = block.reshape(2 * k_one, 2 * k_one) * scale
        high, low = split_high_low(np.kron(square, np.eye(rows)))
        tables.append(jnp.concatenate((high, low) if sign > 0 else (high, low, high), 1))
    return tables


def turned(value, part, length, sign):
    re, im = value
    if part == 0:
        return value
    if 4 * part == length:
        return (-im, re) if sign > 0 else (im, -re)
    cosine = math.cos(2.0 * math.pi * part / length)
    sine = sign * math.sin(2.0 * math.pi * part / length)
    return cosine * re - sine * im, sine * re + cosine * im


def turns(values, sign):
    length = len(values)
    if length == 1:
        return values
    if length % 2:
        sums = []
        for r in range(length):
            terms = [turned(v, k * r % length, length, sign) for k, v in enumerate(values)]
            sums.append((sum(t[0] for t in terms), sum(t[1] for t in terms)))
        return sums
    even, odd = turns(values[::2], sign), turns(values[1::2], sign)
    odd = [turned(v, r, length, sign) for r, v in enumerate(odd)]
    pairs = list(zip(even, odd))
    return [(a[0] + b[0], a[1] + b[1]) for a, b in pairs] + [
        (a[0] - b[0], a[1] - b[1]) for a, b in pairs
    ]


def own_index(kcols):
    return lax.axis_index("krow") * kcols + lax.axis_index("kcol")


def fourier_kernel(kcols, relative, x_ref, w_ref, fwd_ref, inv_ref, o_ref, *scratch):
    devices, energies, _, kcol_each, rows, width = x_ref.shape
    k_one = devices // kcols
    size = k_one * 2 * rows
    me = own_index(kcols) if relative else 0
    spots = [(c, k) for c in range(kcols) for k in range(kcol_each)]
    held = scratch[0] if scratch else o_ref
    copies = []

    def slot(one, c):
        place = one * kcols + c
        return place ^ me if relative else place

    def load(c, e, k):
        parts = [x_ref[slot(one, c), e, :, k] for one in range(k_one)]
        return jnp.stack(parts, 0).reshape(size, width)

    def store(c, e, k, value):
        for one in range(k_one):
            held[slot(one, c), e, :, k] = value[one]

    for e in range(energies):
        state = []
        for c, k in spots:
            block = load(c, e, k)
            block = jnp.concatenate((block, block), 0)
            out = jnp.dot(fwd_ref[...], block, preferred_element_type=jnp.float32)
            out = out.reshape(k_one, 2, rows, width)
            state.append((out[:, 0], out[:, 1]))
        state = turns(state, 1)
        state = [(w_ref[:, r] * re, w_ref[:, r] * im) for r, (re, im) in enumerate(state)]
        state = turns(state, -1)
        for (c, k), (re, im) in zip(spots, state):
            block = jnp.stack((re, im), 1).reshape(size, width)
            high = block.astype(jnp.bfloat16)
            low = (block - high.astype(jnp.float32)).astype(jnp.bfloat16)
            block = jnp.concatenate((high, high, low), 0)
            out = jnp.dot(inv_ref[...], block, preferred_element_type=jnp.float32)
            store(c, e, k, out.astype(jnp.bfloat16).reshape(k_one, 2, rows, width))
        if scratch:
            copies.append(
                pltpu.make_async_copy(held.at[:, e], o_ref.at[:, e], scratch[1].at[e])
            )
            copies[-1].start()
    for copy in copies:
        copy.wait()


LOCAL = pl.BlockSpec(memory_space=pltpu.VMEM)


PARAMS = pltpu.CompilerParams(vmem_limit_bytes=16 * 2**20)


def near(value):
    return pltpu.with_memory_space_constraint(value, pltpu.VMEM)


def far(value):
    return pltpu.with_memory_space_constraint(value, pltpu.HBM)


def fourier(pieces, weights, kcols, relative):
    _, energies, parts, _, rows, width = pieces.shape
    k_one, k_two = weights.shape[:2]
    forward, inverse = row_tables(k_one, k_two, rows)
    size = k_one * parts * rows
    return pl.pallas_call(
        functools.partial(fourier_kernel, kcols, relative),
        in_specs=[LOCAL] * 4,
        out_specs=pl.BlockSpec(memory_space=pltpu.VMEM if relative else pltpu.HBM),
        out_shape=(pltpu.VMEM if relative else pltpu.HBM)(pieces.shape, jnp.bfloat16),
        cost_estimate=pl.CostEstimate(
            flops=2 * 5 * size * size * width * k_two * energies,
            bytes_accessed=4 * pieces.size + 4 * weights.size,
            transcendentals=0,
        ),
        scratch_shapes=()
        if relative
        else [pltpu.VMEM(pieces.shape, jnp.bfloat16), pltpu.SemaphoreType.DMA((energies,))],
        compiler_params=PARAMS,
    )(near(pieces), near(weights), near(forward), near(inverse))


def gather_kernel(g_ref, o_ref, held, sems, out_sems):
    _, energies, parts, each = held.shape[:4]
    spots = [(p, k) for p in range(parts) for k in range(each)]
    inward = [
        [
            pltpu.make_async_copy(
                g_ref.at[e, p, k], held.at[:, e, p, k], sems.at[e, n]
            )
            for n, (p, k) in enumerate(spots)
        ]
        for e in range(energies)
    ]
    outward = [
        pltpu.make_async_copy(held.at[:, e], o_ref.at[:, e], out_sems.at[e])
        for e in range(energies)
    ]
    for copies in inward:
        for copy in copies:
            copy.start()
    for copies, last in zip(inward, outward):
        for copy in copies:
            copy.wait()
        last.start()
    for last in outward:
        last.wait()


def by_device(blocks, energies):
    _, parts, each, devices, rows, width = blocks.shape
    shape = (devices, energies, parts, each, rows, width)
    return pl.pallas_call(
        gather_kernel,
        in_specs=[pl.BlockSpec(memory_space=pltpu.HBM)],
        out_specs=pl.BlockSpec(memory_space=pltpu.HBM),
        out_shape=pltpu.HBM(shape, blocks.dtype),
        scratch_shapes=[
            pltpu.VMEM(shape, blocks.dtype),
            pltpu.SemaphoreType.DMA((energies, parts * each)),
            pltpu.SemaphoreType.DMA((energies,)),
        ],
        compiler_params=PARAMS,
        name="by_device",
    )(far(blocks))


def offset_kernel(first, kcols, g_ref, *refs):
    held, sems = refs[-2:]
    outs = refs[:-2]
    energies, parts, each, devices = held.shape[:4]
    spots = [(e, p, k) for e in range(energies) for p in range(parts) for k in range(each)]
    copies = [
        pltpu.make_async_copy(g_ref.at[first + e, p, k], held.at[e, p, k], sems.at[n])
        for n, (e, p, k) in enumerate(spots)
    ]
    for copy in copies:
        copy.start()
    me = own_index(kcols)
    share = devices // len(outs)
    for copy, (e, p, k) in zip(copies, spots):
        copy.wait()
        for j in range(devices):
            outs[j // share][j % share, e, p, k] = held[e, p, k, j ^ me]


def by_offset(blocks, first, energies, kcols, pieces):
    _, parts, each, devices, rows, width = blocks.shape
    shape = (devices // pieces, energies, parts, each, rows, width)
    return pl.pallas_call(
        functools.partial(offset_kernel, first, kcols),
        in_specs=[pl.BlockSpec(memory_space=pltpu.HBM)],
        out_specs=[LOCAL] * pieces,
        out_shape=[pltpu.VMEM(shape, blocks.dtype)] * pieces,
        scratch_shapes=[
            pltpu.VMEM((energies,) + blocks.shape[1:], blocks.dtype),
            pltpu.SemaphoreType.DMA((energies * parts * each,)),
        ],
        compiler_params=PARAMS,
        name="by_offset",
    )(far(blocks))


def dyson_kernel(first, kcols, relative, s_ref, g_ref, *refs):
    so_ref, d_ref, s_held, d_held, s_sems, d_sems = refs[-6:]
    devices, energies, parts, each, _, orbitals = s_ref.shape
    me = own_index(kcols) if relative else 0
    copies = []

    def send(source, target, sem):
        copies.append(pltpu.make_async_copy(source, target, sem))
        copies[-1].start()

    def product(ar, ai, br, bi):
        right = jnp.concatenate((br, bi), 0)
        dot = lambda left: jnp.dot(left, right, preferred_element_type=jnp.float32)
        return dot(jnp.concatenate((ar, -ai), 1)), dot(jnp.concatenate((ai, ar), 1))

    spots = [(e, k) for e in range(energies) for k in range(each)]
    if relative:
        for d in range(devices):
            s_held[d] = s_ref[d ^ me]
    whole_ref = s_held if relative else s_ref
    for e, k in spots:
        for p in range(parts):
            source = whole_ref.at[:, e, p, k]
            send(source, so_ref.at[first + e, p, k], s_sems.at[e, p, k])
    for e, k in spots:
        load = lambda p: whole_ref[:, e, p, k]
        sr, si = (load(p).reshape(orbitals, orbitals) for p in range(2))
        gr, gi = g_ref[e, 0, 0, k], g_ref[e, 1, 0, k]
        kr, ki = (a.astype(jnp.bfloat16) for a in product(gr, gi, sr, si))
        out = product(kr, ki, gr, gi)
        for p, (whole, change) in enumerate(zip((gr, gi), out)):
            whole = whole.astype(jnp.float32) + change * (1.0 / orbitals)
            d_held[e, p, k] = whole.astype(jnp.bfloat16)
            send(d_held.at[e, p, k], d_ref.at[first + e, p, 0, k], d_sems.at[e, p, k])
    for copy in copies:
        copy.wait()


def dyson(pieces, green, first, kcols, relative, earlier):
    devices, energies, parts, each, rows, orbitals = pieces.shape
    own = green[first : first + energies]
    split = (energies, parts, each, devices, rows, orbitals)
    far_spec = pl.BlockSpec(memory_space=pltpu.HBM)
    return pl.pallas_call(
        functools.partial(dyson_kernel, first, kcols, relative),
        in_specs=[LOCAL, LOCAL] + [far_spec] * len(earlier),
        out_specs=[far_spec, far_spec],
        out_shape=[
            pltpu.HBM((green.shape[0],) + split[1:], jnp.bfloat16),
            pltpu.HBM(green.shape, jnp.bfloat16),
        ],
        input_output_aliases={2 + n: n for n in range(len(earlier))},
        scratch_shapes=[
            pltpu.VMEM(pieces.shape if relative else (1,) * 5 + (orbitals,), jnp.bfloat16),
            pltpu.VMEM(split[:3] + (orbitals, orbitals), jnp.bfloat16),
            pltpu.SemaphoreType.DMA(split[:3]),
            pltpu.SemaphoreType.DMA(split[:3]),
        ],
        cost_estimate=pl.CostEstimate(
            flops=16 * orbitals**3 * each * energies,
            bytes_accessed=16 * pieces.size,
            transcendentals=0,
        ),
        compiler_params=PARAMS,
    )(near(pieces), near(own), *earlier)


def exchange(blocks):
    return lax.all_to_all(blocks, AXES, split_axis=0, concat_axis=0, tiled=True)


def swap(pieces, dims):
    counts, devices = pieces.counts, math.prod(pieces.counts)
    strides = [math.prod(counts[d + 1 :]) for d in range(len(counts))]

    def level(part, left, offset):
        if not left:
            if offset == 0:
                return part
            pairs = [(d, d ^ offset) for d in range(devices)]
            return lax.ppermute(part, AXES, pairs)
        dim, rest = left[0], left[1:]
        cut = part
        if not isinstance(part, (list, tuple)):
            cut = [lax.slice_in_dim(part, q, q + 1, axis=dim) for q in range(counts[dim])]
        back = [level(c, rest, offset + q * strides[dim]) for q, c in enumerate(cut)]
        return lax.concatenate(back, dim)

    return Side(counts, level(pieces.blocks, dims, 0))


class Side(typing.NamedTuple):
    counts: tuple
    blocks: typing.Any

    def merged(self):
        return self.blocks.reshape((-1,) + self.blocks.shape[len(self.counts) :])

    @classmethod
    def of(cls, counts, blocks):
        return cls(counts, blocks.reshape(counts + blocks.shape[1:]))


def per_device(green, screened):
    krows, kcols = lax.axis_size("krow"), lax.axis_size("kcol")
    devices = krows * kcols
    energies, parts, _, each, orbitals, width = green.shape
    rows = orbitals // devices
    weights = screened.reshape(screened.shape[:2] + (rows, width))
    blocks = green.reshape(energies, parts, each, devices, rows, width)
    aside = 1 if kcols == 2 and krows in (8, 16) and energies > 1 else 0
    main = energies - aside
    earlier = ()
    if aside:
        counts = (krows // 8, 2, 2, 2, kcols)
        cut = by_offset(blocks, main, aside, kcols, 2 * counts[0])
        cut = [c.reshape((1, 1) + counts[2:] + c.shape[1:]) for c in cut]
        side = Side(counts, [cut[2 * h : 2 * h + 2] for h in range(counts[0])])
        side = swap(side, (0, 1))
        side = swap(side, (3,))
        side = swap(side, (2, 4))
        turned = fourier(side.merged(), weights, kcols, True)
        side = swap(Side.of(counts, turned), (2,))
        side = swap(side, (0, 1))
        side = swap(side, (3,))
        side = swap(side, (4,))
        earlier = dyson(side.merged(), green, main, kcols, True, ())
    middle = exchange(by_device(blocks, main))
    middle = fourier(middle, weights, kcols, False)
    middle = exchange(middle)
    sigma, dressed = dyson(middle, green, 0, kcols, False, earlier)
    return sigma.reshape(green.shape), dressed


def solution(mesh):
    spec = P(None, None, "krow", "kcol", None, None)
    return jax.shard_map(
        per_device,
        mesh=mesh,
        in_specs=(spec, P(None, None, AXES)),
        out_specs=(spec, spec),
        check_vma=False,
    )
```

```python
import functools
import math
import typing

import jax
import jax.numpy as jnp
import numpy as np
from jax import lax
from jax.experimental import pallas as pl
from jax.experimental.pallas import tpu as pltpu
from jax.sharding import PartitionSpec as P


AXES = ("krow", "kcol")


def phase(length, sign):
    step = np.arange(length)
    angle = 2.0 * math.pi * (step[:, None] * step[None, :] % length) / length
    return np.cos(angle), sign * np.sin(angle)


def split_high_low(table):
    high = jnp.asarray(table, jnp.float32).astype(jnp.bfloat16)
    rest = jnp.asarray(table, jnp.float32) - high.astype(jnp.float32)
    return high, rest.astype(jnp.bfloat16)


def row_tables(k_one, k_two, rows):
    tables = []
    for sign, scale in ((1.0, -1.0 / (k_one * k_two)), (-1.0, 1.0)):
        cosine, sine = phase(k_one, sign)
        block = np.empty((k_one, 2, k_one, 2))
        block[:, 0, :, 0] = cosine
        block[:, 0, :, 1] = -sine
        block[:, 1, :, 0] = sine
        block[:, 1, :, 1] = cosine
        square = block.reshape(2 * k_one, 2 * k_one) * scale
        high, low = split_high_low(np.kron(square, np.eye(rows)))
        tables.append(jnp.concatenate((high, low) if sign > 0 else (high, low, high), 1))
    return tables


def turned(value, part, length, sign):
    re, im = value
    if part == 0:
        return value
    if 4 * part == length:
        return (-im, re) if sign > 0 else (im, -re)
    cosine = math.cos(2.0 * math.pi * part / length)
    sine = sign * math.sin(2.0 * math.pi * part / length)
    return cosine * re - sine * im, sine * re + cosine * im


def turns(values, sign):
    length = len(values)
    if length == 1:
        return values
    if length % 2:
        sums = []
        for r in range(length):
            terms = [turned(v, k * r % length, length, sign) for k, v in enumerate(values)]
            sums.append((sum(t[0] for t in terms), sum(t[1] for t in terms)))
        return sums
    even, odd = turns(values[::2], sign), turns(values[1::2], sign)
    odd = [turned(v, r, length, sign) for r, v in enumerate(odd)]
    pairs = list(zip(even, odd))
    return [(a[0] + b[0], a[1] + b[1]) for a, b in pairs] + [
        (a[0] - b[0], a[1] - b[1]) for a, b in pairs
    ]


def own_index(kcols):
    return lax.axis_index("krow") * kcols + lax.axis_index("kcol")


def fourier_kernel(kcols, relative, x_ref, w_ref, fwd_ref, inv_ref, o_ref, *scratch):
    devices, energies, _, kcol_each, rows, width = x_ref.shape
    k_one = devices // kcols
    size = k_one * 2 * rows
    me = own_index(kcols) if relative else 0
    spots = [(c, k) for c in range(kcols) for k in range(kcol_each)]
    held = scratch[0] if scratch else o_ref
    copies = []

    def slot(one, c):
        place = one * kcols + c
        return place ^ me if relative else place

    def load(c, e, k):
        parts = [x_ref[slot(one, c), e, :, k] for one in range(k_one)]
        return jnp.stack(parts, 0).reshape(size, width)

    def store(c, e, k, value):
        for one in range(k_one):
            held[slot(one, c), e, :, k] = value[one]

    for e in range(energies):
        state = []
        for c, k in spots:
            block = load(c, e, k)
            block = jnp.concatenate((block, block), 0)
            out = jnp.dot(fwd_ref[...], block, preferred_element_type=jnp.float32)
            out = out.reshape(k_one, 2, rows, width)
            state.append((out[:, 0], out[:, 1]))
        state = turns(state, 1)
        state = [(w_ref[:, r] * re, w_ref[:, r] * im) for r, (re, im) in enumerate(state)]
        state = turns(state, -1)
        for (c, k), (re, im) in zip(spots, state):
            block = jnp.stack((re, im), 1).reshape(size, width)
            high = block.astype(jnp.bfloat16)
            low = (block - high.astype(jnp.float32)).astype(jnp.bfloat16)
            block = jnp.concatenate((high, high, low), 0)
            out = jnp.dot(inv_ref[...], block, preferred_element_type=jnp.float32)
            store(c, e, k, out.astype(jnp.bfloat16).reshape(k_one, 2, rows, width))
        if scratch:
            copies.append(
                pltpu.make_async_copy(held.at[:, e], o_ref.at[:, e], scratch[1].at[e])
            )
            copies[-1].start()
    for copy in copies:
        copy.wait()


LOCAL = pl.BlockSpec(memory_space=pltpu.VMEM)


PARAMS = pltpu.CompilerParams(vmem_limit_bytes=16 * 2**20)


def near(value):
    return pltpu.with_memory_space_constraint(value, pltpu.VMEM)


def far(value):
    return pltpu.with_memory_space_constraint(value, pltpu.HBM)


def fourier(pieces, weights, kcols, relative):
    _, energies, parts, _, rows, width = pieces.shape
    k_one, k_two = weights.shape[:2]
    forward, inverse = row_tables(k_one, k_two, rows)
    size = k_one * parts * rows
    return pl.pallas_call(
        functools.partial(fourier_kernel, kcols, relative),
        in_specs=[LOCAL] * 4,
        out_specs=pl.BlockSpec(memory_space=pltpu.VMEM if relative else pltpu.HBM),
        out_shape=(pltpu.VMEM if relative else pltpu.HBM)(pieces.shape, jnp.bfloat16),
        cost_estimate=pl.CostEstimate(
            flops=2 * 5 * size * size * width * k_two * energies,
            bytes_accessed=4 * pieces.size + 4 * weights.size,
            transcendentals=0,
        ),
        scratch_shapes=()
        if relative
        else [pltpu.VMEM(pieces.shape, jnp.bfloat16), pltpu.SemaphoreType.DMA((energies,))],
        compiler_params=PARAMS,
    )(near(pieces), near(weights), near(forward), near(inverse))


def gather_kernel(g_ref, o_ref, held, sems, out_sems):
    _, energies, parts, each = held.shape[:4]
    spots = [(p, k) for p in range(parts) for k in range(each)]
    inward = [
        [
            pltpu.make_async_copy(
                g_ref.at[e, p, k], held.at[:, e, p, k], sems.at[e, n]
            )
            for n, (p, k) in enumerate(spots)
        ]
        for e in range(energies)
    ]
    outward = [
        pltpu.make_async_copy(held.at[:, e], o_ref.at[:, e], out_sems.at[e])
        for e in range(energies)
    ]
    for copies in inward:
        for copy in copies:
            copy.start()
    for copies, last in zip(inward, outward):
        for copy in copies:
            copy.wait()
        last.start()
    for last in outward:
        last.wait()


def by_device(blocks, energies):
    _, parts, each, devices, rows, width = blocks.shape
    shape = (devices, energies, parts, each, rows, width)
    return pl.pallas_call(
        gather_kernel,
        in_specs=[pl.BlockSpec(memory_space=pltpu.HBM)],
        out_specs=pl.BlockSpec(memory_space=pltpu.HBM),
        out_shape=pltpu.HBM(shape, blocks.dtype),
        scratch_shapes=[
            pltpu.VMEM(shape, blocks.dtype),
            pltpu.SemaphoreType.DMA((energies, parts * each)),
            pltpu.SemaphoreType.DMA((energies,)),
        ],
        compiler_params=PARAMS,
        name="by_device",
    )(far(blocks))


def offset_kernel(first, kcols, g_ref, *refs):
    held, sems = refs[-2:]
    outs = refs[:-2]
    energies, parts, each, devices = held.shape[:4]
    spots = [(e, p, k) for e in range(energies) for p in range(parts) for k in range(each)]
    copies = [
        pltpu.make_async_copy(g_ref.at[first + e, p, k], held.at[e, p, k], sems.at[n])
        for n, (e, p, k) in enumerate(spots)
    ]
    for copy in copies:
        copy.start()
    me = own_index(kcols)
    share = devices // len(outs)
    for copy, (e, p, k) in zip(copies, spots):
        copy.wait()
        for j in range(devices):
            outs[j // share][j % share, e, p, k] = held[e, p, k, j ^ me]


def by_offset(blocks, first, energies, kcols, pieces):
    _, parts, each, devices, rows, width = blocks.shape
    shape = (devices // pieces, energies, parts, each, rows, width)
    return pl.pallas_call(
        functools.partial(offset_kernel, first, kcols),
        in_specs=[pl.BlockSpec(memory_space=pltpu.HBM)],
        out_specs=[LOCAL] * pieces,
        out_shape=[pltpu.VMEM(shape, blocks.dtype)] * pieces,
        scratch_shapes=[
            pltpu.VMEM((energies,) + blocks.shape[1:], blocks.dtype),
            pltpu.SemaphoreType.DMA((energies * parts * each,)),
        ],
        compiler_params=PARAMS,
        name="by_offset",
    )(far(blocks))


def dyson_kernel(first, kcols, relative, s_ref, g_ref, *refs):
    so_ref, d_ref, s_held, d_held, s_sems, d_sems = refs[-6:]
    devices, energies, parts, each, _, orbitals = s_ref.shape
    me = own_index(kcols) if relative else 0
    copies = []

    def send(source, target, sem):
        copies.append(pltpu.make_async_copy(source, target, sem))
        copies[-1].start()

    def product(ar, ai, br, bi):
        right = jnp.concatenate((br, bi), 0)
        dot = lambda left: jnp.dot(left, right, preferred_element_type=jnp.float32)
        return dot(jnp.concatenate((ar, -ai), 1)), dot(jnp.concatenate((ai, ar), 1))

    spots = [(e, k) for e in range(energies) for k in range(each)]
    if relative:
        for d in range(devices):
            s_held[d] = s_ref[d ^ me]
    whole_ref = s_held if relative else s_ref
    for e, k in spots:
        for p in range(parts):
            source = whole_ref.at[:, e, p, k]
            send(source, so_ref.at[first + e, p, k], s_sems.at[e, p, k])

    def first_product(e, k):
        sr, si = (whole_ref[:, e, p, k].reshape(orbitals, orbitals) for p in range(2))
        out = product(g_ref[e, 0, 0, k], g_ref[e, 1, 0, k], sr, si)
        return [a.astype(jnp.bfloat16) for a in out]

    ahead = [first_product(*spots[0])]
    for n, (e, k) in enumerate(spots):
        if n + 1 < len(spots):
            ahead.append(first_product(*spots[n + 1]))
        green = g_ref[e, 0, 0, k], g_ref[e, 1, 0, k]
        out = product(*ahead[n], *green)
        for p, (whole, change) in enumerate(zip(green, out)):
            whole = whole.astype(jnp.float32) + change * (1.0 / orbitals)
            d_held[e, p, k] = whole.astype(jnp.bfloat16)
        for p in range(parts):
            send(d_held.at[e, p, k], d_ref.at[first + e, p, 0, k], d_sems.at[e, p, k])
    for copy in copies:
        copy.wait()


def dyson(pieces, green, first, kcols, relative, earlier):
    devices, energies, parts, each, rows, orbitals = pieces.shape
    own = green[first : first + energies]
    split = (energies, parts, each, devices, rows, orbitals)
    far_spec = pl.BlockSpec(memory_space=pltpu.HBM)
    return pl.pallas_call(
        functools.partial(dyson_kernel, first, kcols, relative),
        in_specs=[LOCAL, LOCAL] + [far_spec] * len(earlier),
        out_specs=[far_spec, far_spec],
        out_shape=[
            pltpu.HBM((green.shape[0],) + split[1:], jnp.bfloat16),
            pltpu.HBM(green.shape, jnp.bfloat16),
        ],
        input_output_aliases={2 + n: n for n in range(len(earlier))},
        scratch_shapes=[
            pltpu.VMEM(pieces.shape if relative else (1,) * 5 + (orbitals,), jnp.bfloat16),
            pltpu.VMEM(split[:3] + (orbitals, orbitals), jnp.bfloat16),
            pltpu.SemaphoreType.DMA(split[:3]),
            pltpu.SemaphoreType.DMA(split[:3]),
        ],
        cost_estimate=pl.CostEstimate(
            flops=16 * orbitals**3 * each * energies,
            bytes_accessed=16 * pieces.size,
            transcendentals=0,
        ),
        compiler_params=PARAMS,
    )(near(pieces), near(own), *earlier)


def exchange(blocks):
    return lax.all_to_all(blocks, AXES, split_axis=0, concat_axis=0, tiled=True)


def swap(pieces, dims):
    counts, devices = pieces.counts, math.prod(pieces.counts)
    strides = [math.prod(counts[d + 1 :]) for d in range(len(counts))]

    def level(part, left, offset):
        if not left:
            if offset == 0:
                return part
            pairs = [(d, d ^ offset) for d in range(devices)]
            return lax.ppermute(part, AXES, pairs)
        dim, rest = left[0], left[1:]
        cut = part
        if not isinstance(part, (list, tuple)):
            cut = [lax.slice_in_dim(part, q, q + 1, axis=dim) for q in range(counts[dim])]
        back = [level(c, rest, offset + q * strides[dim]) for q, c in enumerate(cut)]
        return lax.concatenate(back, dim)

    return Side(counts, level(pieces.blocks, dims, 0))


class Side(typing.NamedTuple):
    counts: tuple
    blocks: typing.Any

    def merged(self):
        return self.blocks.reshape((-1,) + self.blocks.shape[len(self.counts) :])

    @classmethod
    def of(cls, counts, blocks):
        return cls(counts, blocks.reshape(counts + blocks.shape[1:]))


def per_device(green, screened):
    krows, kcols = lax.axis_size("krow"), lax.axis_size("kcol")
    devices = krows * kcols
    energies, parts, _, each, orbitals, width = green.shape
    rows = orbitals // devices
    weights = screened.reshape(screened.shape[:2] + (rows, width))
    blocks = green.reshape(energies, parts, each, devices, rows, width)
    aside = 1 if kcols == 2 and krows in (8, 16) and energies > 1 else 0
    main = energies - aside
    earlier = ()
    if aside:
        counts = (krows // 8, 2, 2, 2, kcols)
        cut = by_offset(blocks, main, aside, kcols, 2 * counts[0])
        cut = [c.reshape((1, 1) + counts[2:] + c.shape[1:]) for c in cut]
        side = Side(counts, [cut[2 * h : 2 * h + 2] for h in range(counts[0])])
        side = swap(side, (0, 1))
        side = swap(side, (3,))
        side = swap(side, (2, 4))
        turned = fourier(side.merged(), weights, kcols, True)
        side = swap(Side.of(counts, turned), (2,))
        side = swap(side, (0, 1))
        side = swap(side, (3,))
        side = swap(side, (4,))
        earlier = dyson(side.merged(), green, main, kcols, True, ())
    middle = exchange(by_device(blocks, main))
    middle = fourier(middle, weights, kcols, False)
    middle = exchange(middle)
    sigma, dressed = dyson(middle, green, 0, kcols, False, earlier)
    return sigma.reshape(green.shape), dressed


def solution(mesh):
    spec = P(None, None, "krow", "kcol", None, None)
    return jax.shard_map(
        per_device,
        mesh=mesh,
        in_specs=(spec, P(None, None, AXES)),
        out_specs=(spec, spec),
        check_vma=False,
    )
```

```python
import functools
import math
import typing

import jax
import jax.numpy as jnp
import numpy as np
from jax import lax
from jax.experimental import pallas as pl
from jax.experimental.pallas import tpu as pltpu
from jax.sharding import PartitionSpec as P


AXES = ("krow", "kcol")


def phase(length, sign):
    step = np.arange(length)
    angle = 2.0 * math.pi * (step[:, None] * step[None, :] % length) / length
    return np.cos(angle), sign * np.sin(angle)


def split_high_low(table):
    high = jnp.asarray(table, jnp.float32).astype(jnp.bfloat16)
    rest = jnp.asarray(table, jnp.float32) - high.astype(jnp.float32)
    return high, rest.astype(jnp.bfloat16)


def row_tables(k_one, k_two, rows):
    tables = []
    for sign, scale in ((1.0, -1.0 / (k_one * k_two)), (-1.0, 1.0)):
        cosine, sine = phase(k_one, sign)
        block = np.empty((k_one, 2, k_one, 2))
        block[:, 0, :, 0] = cosine
        block[:, 0, :, 1] = -sine
        block[:, 1, :, 0] = sine
        block[:, 1, :, 1] = cosine
        square = block.reshape(2 * k_one, 2 * k_one) * scale
        high, low = split_high_low(np.kron(square, np.eye(rows)))
        tables.append(jnp.concatenate((high, low) if sign > 0 else (high, low, high), 1))
    return tables


def turned(value, part, length, sign):
    re, im = value
    if part == 0:
        return value
    if 4 * part == length:
        return (-im, re) if sign > 0 else (im, -re)
    cosine = math.cos(2.0 * math.pi * part / length)
    sine = sign * math.sin(2.0 * math.pi * part / length)
    return cosine * re - sine * im, sine * re + cosine * im


def turns(values, sign):
    length = len(values)
    if length == 1:
        return values
    if length % 2:
        sums = []
        for r in range(length):
            terms = [turned(v, k * r % length, length, sign) for k, v in enumerate(values)]
            sums.append((sum(t[0] for t in terms), sum(t[1] for t in terms)))
        return sums
    even, odd = turns(values[::2], sign), turns(values[1::2], sign)
    odd = [turned(v, r, length, sign) for r, v in enumerate(odd)]
    pairs = list(zip(even, odd))
    return [(a[0] + b[0], a[1] + b[1]) for a, b in pairs] + [
        (a[0] - b[0], a[1] - b[1]) for a, b in pairs
    ]


def own_index(kcols):
    return lax.axis_index("krow") * kcols + lax.axis_index("kcol")


def fourier_kernel(kcols, relative, x_ref, w_ref, fwd_ref, inv_ref, o_ref, *scratch):
    devices, energies, _, kcol_each, rows, width = x_ref.shape
    k_one = devices // kcols
    size = k_one * 2 * rows
    me = own_index(kcols) if relative else 0
    spots = [(c, k) for c in range(kcols) for k in range(kcol_each)]
    held = scratch[0] if scratch else o_ref
    copies = []

    def slot(one, c):
        place = one * kcols + c
        return place ^ me if relative else place

    def load(c, e, k):
        parts = [x_ref[slot(one, c), e, :, k] for one in range(k_one)]
        return jnp.stack(parts, 0).reshape(size, width)

    def store(c, e, k, value):
        for one in range(k_one):
            held[slot(one, c), e, :, k] = value[one]

    def forward(e):
        state = []
        for c, k in spots:
            block = load(c, e, k)
            block = jnp.concatenate((block, block), 0)
            out = jnp.dot(fwd_ref[...], block, preferred_element_type=jnp.float32)
            out = out.reshape(k_one, 2, rows, width)
            state.append((out[:, 0], out[:, 1]))
        return state

    ahead = [forward(0)]
    for e in range(energies):
        state = turns(ahead[e], 1)
        state = [(w_ref[:, r] * re, w_ref[:, r] * im) for r, (re, im) in enumerate(state)]
        state = turns(state, -1)
        if e + 1 < energies:
            ahead.append(forward(e + 1))
        for (c, k), (re, im) in zip(spots, state):
            block = jnp.stack((re, im), 1).reshape(size, width)
            high = block.astype(jnp.bfloat16)
            low = (block - high.astype(jnp.float32)).astype(jnp.bfloat16)
            block = jnp.concatenate((high, high, low), 0)
            out = jnp.dot(inv_ref[...], block, preferred_element_type=jnp.float32)
            store(c, e, k, out.astype(jnp.bfloat16).reshape(k_one, 2, rows, width))
        if scratch:
            copies.append(
                pltpu.make_async_copy(held.at[:, e], o_ref.at[:, e], scratch[1].at[e])
            )
            copies[-1].start()
    for copy in copies:
        copy.wait()


LOCAL = pl.BlockSpec(memory_space=pltpu.VMEM)


PARAMS = pltpu.CompilerParams(vmem_limit_bytes=16 * 2**20)


def near(value):
    return pltpu.with_memory_space_constraint(value, pltpu.VMEM)


def far(value):
    return pltpu.with_memory_space_constraint(value, pltpu.HBM)


def fourier(pieces, weights, kcols, relative):
    _, energies, parts, _, rows, width = pieces.shape
    k_one, k_two = weights.shape[:2]
    forward, inverse = row_tables(k_one, k_two, rows)
    size = k_one * parts * rows
    return pl.pallas_call(
        functools.partial(fourier_kernel, kcols, relative),
        in_specs=[LOCAL] * 4,
        out_specs=pl.BlockSpec(memory_space=pltpu.VMEM if relative else pltpu.HBM),
        out_shape=(pltpu.VMEM if relative else pltpu.HBM)(pieces.shape, jnp.bfloat16),
        cost_estimate=pl.CostEstimate(
            flops=2 * 5 * size * size * width * k_two * energies,
            bytes_accessed=4 * pieces.size + 4 * weights.size,
            transcendentals=0,
        ),
        scratch_shapes=()
        if relative
        else [pltpu.VMEM(pieces.shape, jnp.bfloat16), pltpu.SemaphoreType.DMA((energies,))],
        compiler_params=PARAMS,
    )(near(pieces), near(weights), near(forward), near(inverse))


def gather_kernel(g_ref, o_ref, held, sems, out_sems):
    _, energies, parts, each = held.shape[:4]
    spots = [(p, k) for p in range(parts) for k in range(each)]
    inward = [
        [
            pltpu.make_async_copy(
                g_ref.at[e, p, k], held.at[:, e, p, k], sems.at[e, n]
            )
            for n, (p, k) in enumerate(spots)
        ]
        for e in range(energies)
    ]
    outward = [
        pltpu.make_async_copy(held.at[:, e], o_ref.at[:, e], out_sems.at[e])
        for e in range(energies)
    ]
    for copies in inward:
        for copy in copies:
            copy.start()
    for copies, last in zip(inward, outward):
        for copy in copies:
            copy.wait()
        last.start()
    for last in outward:
        last.wait()


def by_device(blocks, energies):
    _, parts, each, devices, rows, width = blocks.shape
    shape = (devices, energies, parts, each, rows, width)
    return pl.pallas_call(
        gather_kernel,
        in_specs=[pl.BlockSpec(memory_space=pltpu.HBM)],
        out_specs=pl.BlockSpec(memory_space=pltpu.HBM),
        out_shape=pltpu.HBM(shape, blocks.dtype),
        scratch_shapes=[
            pltpu.VMEM(shape, blocks.dtype),
            pltpu.SemaphoreType.DMA((energies, parts * each)),
            pltpu.SemaphoreType.DMA((energies,)),
        ],
        compiler_params=PARAMS,
        name="by_device",
    )(far(blocks))


def offset_kernel(first, kcols, g_ref, *refs):
    held, sems = refs[-2:]
    outs = refs[:-2]
    energies, parts, each, devices = held.shape[:4]
    spots = [(e, p, k) for e in range(energies) for p in range(parts) for k in range(each)]
    copies = [
        pltpu.make_async_copy(g_ref.at[first + e, p, k], held.at[e, p, k], sems.at[n])
        for n, (e, p, k) in enumerate(spots)
    ]
    for copy in copies:
        copy.start()
    me = own_index(kcols)
    share = devices // len(outs)
    for copy, (e, p, k) in zip(copies, spots):
        copy.wait()
        for j in range(devices):
            outs[j // share][j % share, e, p, k] = held[e, p, k, j ^ me]


def by_offset(blocks, first, energies, kcols, pieces):
    _, parts, each, devices, rows, width = blocks.shape
    shape = (devices // pieces, energies, parts, each, rows, width)
    return pl.pallas_call(
        functools.partial(offset_kernel, first, kcols),
        in_specs=[pl.BlockSpec(memory_space=pltpu.HBM)],
        out_specs=[LOCAL] * pieces,
        out_shape=[pltpu.VMEM(shape, blocks.dtype)] * pieces,
        scratch_shapes=[
            pltpu.VMEM((energies,) + blocks.shape[1:], blocks.dtype),
            pltpu.SemaphoreType.DMA((energies * parts * each,)),
        ],
        compiler_params=PARAMS,
        name="by_offset",
    )(far(blocks))


def dyson_kernel(first, kcols, relative, s_ref, g_ref, *refs):
    so_ref, d_ref, s_held, d_held, s_sems, d_sems = refs[-6:]
    devices, energies, parts, each, _, orbitals = s_ref.shape
    me = own_index(kcols) if relative else 0
    copies = []

    def send(source, target, sem):
        copies.append(pltpu.make_async_copy(source, target, sem))
        copies[-1].start()

    def product(ar, ai, br, bi):
        right = jnp.concatenate((br, bi), 0)
        dot = lambda left: jnp.dot(left, right, preferred_element_type=jnp.float32)
        return dot(jnp.concatenate((ar, -ai), 1)), dot(jnp.concatenate((ai, ar), 1))

    spots = [(e, k) for e in range(energies) for k in range(each)]
    if relative:
        for d in range(devices):
            s_held[d] = s_ref[d ^ me]
    whole_ref = s_held if relative else s_ref
    for e, k in spots:
        for p in range(parts):
            source = whole_ref.at[:, e, p, k]
            send(source, so_ref.at[first + e, p, k], s_sems.at[e, p, k])

    def first_product(e, k):
        sr, si = (whole_ref[:, e, p, k].reshape(orbitals, orbitals) for p in range(2))
        out = product(g_ref[e, 0, 0, k], g_ref[e, 1, 0, k], sr, si)
        return [a.astype(jnp.bfloat16) for a in out]

    ahead = [first_product(*spots[0])]
    for n, (e, k) in enumerate(spots):
        if n + 1 < len(spots):
            ahead.append(first_product(*spots[n + 1]))
        green = g_ref[e, 0, 0, k], g_ref[e, 1, 0, k]
        out = product(*ahead[n], *green)
        for p, (whole, change) in enumerate(zip(green, out)):
            whole = whole.astype(jnp.float32) + change * (1.0 / orbitals)
            d_held[e, p, k] = whole.astype(jnp.bfloat16)
        for p in range(parts):
            send(d_held.at[e, p, k], d_ref.at[first + e, p, 0, k], d_sems.at[e, p, k])
    for copy in copies:
        copy.wait()


def dyson(pieces, green, first, kcols, relative, earlier):
    devices, energies, parts, each, rows, orbitals = pieces.shape
    own = green[first : first + energies]
    split = (energies, parts, each, devices, rows, orbitals)
    far_spec = pl.BlockSpec(memory_space=pltpu.HBM)
    return pl.pallas_call(
        functools.partial(dyson_kernel, first, kcols, relative),
        in_specs=[LOCAL, LOCAL] + [far_spec] * len(earlier),
        out_specs=[far_spec, far_spec],
        out_shape=[
            pltpu.HBM((green.shape[0],) + split[1:], jnp.bfloat16),
            pltpu.HBM(green.shape, jnp.bfloat16),
        ],
        input_output_aliases={2 + n: n for n in range(len(earlier))},
        scratch_shapes=[
            pltpu.VMEM(pieces.shape if relative else (1,) * 5 + (orbitals,), jnp.bfloat16),
            pltpu.VMEM(split[:3] + (orbitals, orbitals), jnp.bfloat16),
            pltpu.SemaphoreType.DMA(split[:3]),
            pltpu.SemaphoreType.DMA(split[:3]),
        ],
        cost_estimate=pl.CostEstimate(
            flops=16 * orbitals**3 * each * energies,
            bytes_accessed=16 * pieces.size,
            transcendentals=0,
        ),
        compiler_params=PARAMS,
    )(near(pieces), near(own), *earlier)


def exchange(blocks):
    return lax.all_to_all(blocks, AXES, split_axis=0, concat_axis=0, tiled=True)


def swap(pieces, dims):
    counts, devices = pieces.counts, math.prod(pieces.counts)
    strides = [math.prod(counts[d + 1 :]) for d in range(len(counts))]

    def level(part, left, offset):
        if not left:
            if offset == 0:
                return part
            pairs = [(d, d ^ offset) for d in range(devices)]
            return lax.ppermute(part, AXES, pairs)
        dim, rest = left[0], left[1:]
        cut = part
        if not isinstance(part, (list, tuple)):
            cut = [lax.slice_in_dim(part, q, q + 1, axis=dim) for q in range(counts[dim])]
        back = [level(c, rest, offset + q * strides[dim]) for q, c in enumerate(cut)]
        return lax.concatenate(back, dim)

    return Side(counts, level(pieces.blocks, dims, 0))


class Side(typing.NamedTuple):
    counts: tuple
    blocks: typing.Any

    def merged(self):
        return self.blocks.reshape((-1,) + self.blocks.shape[len(self.counts) :])

    @classmethod
    def of(cls, counts, blocks):
        return cls(counts, blocks.reshape(counts + blocks.shape[1:]))


def per_device(green, screened):
    krows, kcols = lax.axis_size("krow"), lax.axis_size("kcol")
    devices = krows * kcols
    energies, parts, _, each, orbitals, width = green.shape
    rows = orbitals // devices
    weights = screened.reshape(screened.shape[:2] + (rows, width))
    blocks = green.reshape(energies, parts, each, devices, rows, width)
    aside = 1 if kcols == 2 and krows in (8, 16) and energies > 1 else 0
    main = energies - aside
    earlier = ()
    if aside:
        counts = (krows // 8, 2, 2, 2, kcols)
        cut = by_offset(blocks, main, aside, kcols, 2 * counts[0])
        cut = [c.reshape((1, 1) + counts[2:] + c.shape[1:]) for c in cut]
        side = Side(counts, [cut[2 * h : 2 * h + 2] for h in range(counts[0])])
        side = swap(side, (0, 1))
        side = swap(side, (3,))
        side = swap(side, (2, 4))
        turned = fourier(side.merged(), weights, kcols, True)
        side = swap(Side.of(counts, turned), (2,))
        side = swap(side, (0, 1))
        side = swap(side, (3,))
        side = swap(side, (4,))
        earlier = dyson(side.merged(), green, main, kcols, True, ())
    middle = exchange(by_device(blocks, main))
    middle = fourier(middle, weights, kcols, False)
    middle = exchange(middle)
    sigma, dressed = dyson(middle, green, 0, kcols, False, earlier)
    return sigma.reshape(green.shape), dressed


def solution(mesh):
    spec = P(None, None, "krow", "kcol", None, None)
    return jax.shard_map(
        per_device,
        mesh=mesh,
        in_specs=(spec, P(None, None, AXES)),
        out_specs=(spec, spec),
        check_vma=False,
    )
```

```python
import functools
import math
import typing

import jax
import jax.numpy as jnp
import numpy as np
from jax import lax
from jax.experimental import pallas as pl
from jax.experimental.pallas import tpu as pltpu
from jax.sharding import PartitionSpec as P


AXES = ("krow", "kcol")


def phase(length, sign):
    step = np.arange(length)
    angle = 2.0 * math.pi * (step[:, None] * step[None, :] % length) / length
    return np.cos(angle), sign * np.sin(angle)


def split_high_low(table):
    high = jnp.asarray(table, jnp.float32).astype(jnp.bfloat16)
    rest = jnp.asarray(table, jnp.float32) - high.astype(jnp.float32)
    return high, rest.astype(jnp.bfloat16)


def row_tables(k_one, k_two, rows):
    tables = []
    for sign, scale in ((1.0, -1.0 / (k_one * k_two)), (-1.0, 1.0)):
        cosine, sine = phase(k_one, sign)
        block = np.empty((k_one, 2, k_one, 2))
        block[:, 0, :, 0] = cosine
        block[:, 0, :, 1] = -sine
        block[:, 1, :, 0] = sine
        block[:, 1, :, 1] = cosine
        square = block.reshape(2 * k_one, 2 * k_one) * scale
        high, low = split_high_low(np.kron(square, np.eye(rows)))
        tables.append(jnp.concatenate((high, low) if sign > 0 else (high, low, high), 1))
    return tables


def turned(value, part, length, sign):
    re, im = value
    if part == 0:
        return value
    if 4 * part == length:
        return (-im, re) if sign > 0 else (im, -re)
    cosine = math.cos(2.0 * math.pi * part / length)
    sine = sign * math.sin(2.0 * math.pi * part / length)
    return cosine * re - sine * im, sine * re + cosine * im


def turns(values, sign):
    length = len(values)
    if length == 1:
        return values
    if length % 2:
        sums = []
        for r in range(length):
            terms = [turned(v, k * r % length, length, sign) for k, v in enumerate(values)]
            sums.append((sum(t[0] for t in terms), sum(t[1] for t in terms)))
        return sums
    even, odd = turns(values[::2], sign), turns(values[1::2], sign)
    odd = [turned(v, r, length, sign) for r, v in enumerate(odd)]
    pairs = list(zip(even, odd))
    return [(a[0] + b[0], a[1] + b[1]) for a, b in pairs] + [
        (a[0] - b[0], a[1] - b[1]) for a, b in pairs
    ]


def own_index(kcols):
    return lax.axis_index("krow") * kcols + lax.axis_index("kcol")


def fourier_kernel(kcols, counts, w_ref, fwd_ref, inv_ref, *refs):
    relative = bool(counts)
    if relative:
        o_ref, x_ref = refs[-2:]
        scratch = ()
        for j, digits in enumerate(np.ndindex(*counts)):
            high, low, x, core, y = digits
            piece = refs[x * counts[4] + y]
            x_ref[j] = piece[(high * counts[1] + low) * counts[3] + core]
    else:
        x_ref, o_ref, *scratch = refs
    devices, energies, _, kcol_each, rows, width = x_ref.shape
    k_one = devices // kcols
    size = k_one * 2 * rows
    me = own_index(kcols) if relative else 0
    spots = [(c, k) for c in range(kcols) for k in range(kcol_each)]
    held = scratch[0] if scratch else o_ref
    copies = []

    def slot(one, c):
        place = one * kcols + c
        return place ^ me if relative else place

    def load(c, e, k):
        parts = [x_ref[slot(one, c), e, :, k] for one in range(k_one)]
        return jnp.stack(parts, 0).reshape(size, width)

    def store(c, e, k, value):
        for one in range(k_one):
            held[slot(one, c), e, :, k] = value[one]

    def forward(e):
        state = []
        for c, k in spots:
            block = load(c, e, k)
            block = jnp.concatenate((block, block), 0)
            out = jnp.dot(fwd_ref[...], block, preferred_element_type=jnp.float32)
            out = out.reshape(k_one, 2, rows, width)
            state.append((out[:, 0], out[:, 1]))
        return state

    ahead = [forward(0)]
    for e in range(energies):
        state = turns(ahead[e], 1)
        state = [(w_ref[:, r] * re, w_ref[:, r] * im) for r, (re, im) in enumerate(state)]
        state = turns(state, -1)
        if e + 1 < energies:
            ahead.append(forward(e + 1))
        for (c, k), (re, im) in zip(spots, state):
            block = jnp.stack((re, im), 1).reshape(size, width)
            high = block.astype(jnp.bfloat16)
            low = (block - high.astype(jnp.float32)).astype(jnp.bfloat16)
            block = jnp.concatenate((high, high, low), 0)
            out = jnp.dot(inv_ref[...], block, preferred_element_type=jnp.float32)
            store(c, e, k, out.astype(jnp.bfloat16).reshape(k_one, 2, rows, width))
        if scratch:
            copies.append(
                pltpu.make_async_copy(held.at[:, e], o_ref.at[:, e], scratch[1].at[e])
            )
            copies[-1].start()
    for copy in copies:
        copy.wait()


LOCAL = pl.BlockSpec(memory_space=pltpu.VMEM)


PARAMS = pltpu.CompilerParams(vmem_limit_bytes=16 * 2**20)


def near(value):
    return pltpu.with_memory_space_constraint(value, pltpu.VMEM)


def far(value):
    return pltpu.with_memory_space_constraint(value, pltpu.HBM)


def fourier(pieces, weights, kcols, counts):
    if counts:
        skip = len(counts)
        pieces = [p.reshape((-1,) + p.shape[skip:]) for row in pieces for p in row]
        shape = (math.prod(counts),) + pieces[0].shape[1:]
        scratch = [pltpu.VMEM(shape, jnp.bfloat16)]
    else:
        pieces, shape = [pieces], pieces.shape
        scratch = [pltpu.VMEM(shape, jnp.bfloat16), pltpu.SemaphoreType.DMA(shape[1:2])]
    _, energies, parts, _, rows, width = shape
    k_one, k_two = weights.shape[:2]
    forward, inverse = row_tables(k_one, k_two, rows)
    size = k_one * parts * rows
    return pl.pallas_call(
        functools.partial(fourier_kernel, kcols, counts),
        in_specs=[LOCAL] * (3 + len(pieces)),
        out_specs=pl.BlockSpec(memory_space=pltpu.VMEM if counts else pltpu.HBM),
        out_shape=(pltpu.VMEM if counts else pltpu.HBM)(shape, jnp.bfloat16),
        cost_estimate=pl.CostEstimate(
            flops=2 * 5 * size * size * width * k_two * energies,
            bytes_accessed=4 * math.prod(shape) + 4 * weights.size,
            transcendentals=0,
        ),
        scratch_shapes=scratch,
        compiler_params=PARAMS,
    )(near(weights), near(forward), near(inverse), *map(near, pieces))


def gather_kernel(g_ref, o_ref, held, sems, out_sems):
    _, energies, parts, each = held.shape[:4]
    spots = [(p, k) for p in range(parts) for k in range(each)]
    inward = [
        [
            pltpu.make_async_copy(
                g_ref.at[e, p, k], held.at[:, e, p, k], sems.at[e, n]
            )
            for n, (p, k) in enumerate(spots)
        ]
        for e in range(energies)
    ]
    outward = [
        pltpu.make_async_copy(held.at[:, e], o_ref.at[:, e], out_sems.at[e])
        for e in range(energies)
    ]
    for copies in inward:
        for copy in copies:
            copy.start()
    for copies, last in zip(inward, outward):
        for copy in copies:
            copy.wait()
        last.start()
    for last in outward:
        last.wait()


def by_device(blocks, energies):
    _, parts, each, devices, rows, width = blocks.shape
    shape = (devices, energies, parts, each, rows, width)
    return pl.pallas_call(
        gather_kernel,
        in_specs=[pl.BlockSpec(memory_space=pltpu.HBM)],
        out_specs=pl.BlockSpec(memory_space=pltpu.HBM),
        out_shape=pltpu.HBM(shape, blocks.dtype),
        scratch_shapes=[
            pltpu.VMEM(shape, blocks.dtype),
            pltpu.SemaphoreType.DMA((energies, parts * each)),
            pltpu.SemaphoreType.DMA((energies,)),
        ],
        compiler_params=PARAMS,
        name="by_device",
    )(far(blocks))


def offset_kernel(first, kcols, g_ref, *refs):
    held, sems = refs[-2:]
    outs = refs[:-2]
    energies, parts, each, devices = held.shape[:4]
    spots = [(e, p, k) for e in range(energies) for p in range(parts) for k in range(each)]
    copies = [
        pltpu.make_async_copy(g_ref.at[first + e, p, k], held.at[e, p, k], sems.at[n])
        for n, (e, p, k) in enumerate(spots)
    ]
    for copy in copies:
        copy.start()
    me = own_index(kcols)
    share = devices // len(outs)
    for copy, (e, p, k) in zip(copies, spots):
        copy.wait()
        for j in range(devices):
            outs[j // share][j % share, e, p, k] = held[e, p, k, j ^ me]


def by_offset(blocks, first, energies, kcols, pieces):
    _, parts, each, devices, rows, width = blocks.shape
    shape = (devices // pieces, energies, parts, each, rows, width)
    return pl.pallas_call(
        functools.partial(offset_kernel, first, kcols),
        in_specs=[pl.BlockSpec(memory_space=pltpu.HBM)],
        out_specs=[LOCAL] * pieces,
        out_shape=[pltpu.VMEM(shape, blocks.dtype)] * pieces,
        scratch_shapes=[
            pltpu.VMEM((energies,) + blocks.shape[1:], blocks.dtype),
            pltpu.SemaphoreType.DMA((energies * parts * each,)),
        ],
        compiler_params=PARAMS,
        name="by_offset",
    )(far(blocks))


def dyson_kernel(first, kcols, relative, s_ref, g_ref, *refs):
    so_ref, d_ref, s_held, d_held, s_sems, d_sems = refs[-6:]
    devices, energies, parts, each, _, orbitals = s_ref.shape
    me = own_index(kcols) if relative else 0
    copies = []

    def send(source, target, sem):
        copies.append(pltpu.make_async_copy(source, target, sem))
        copies[-1].start()

    def product(ar, ai, br, bi):
        right = jnp.concatenate((br, bi), 0)
        dot = lambda left: jnp.dot(left, right, preferred_element_type=jnp.float32)
        return dot(jnp.concatenate((ar, -ai), 1)), dot(jnp.concatenate((ai, ar), 1))

    spots = [(e, k) for e in range(energies) for k in range(each)]
    if relative:
        for d in range(devices):
            s_held[d] = s_ref[d ^ me]
    whole_ref = s_held if relative else s_ref
    for e, k in spots:
        for p in range(parts):
            source = whole_ref.at[:, e, p, k]
            send(source, so_ref.at[first + e, p, k], s_sems.at[e, p, k])

    def first_product(e, k):
        sr, si = (whole_ref[:, e, p, k].reshape(orbitals, orbitals) for p in range(2))
        out = product(g_ref[e, 0, 0, k], g_ref[e, 1, 0, k], sr, si)
        return [a.astype(jnp.bfloat16) for a in out]

    ahead = [first_product(*spots[0])]
    for n, (e, k) in enumerate(spots):
        if n + 1 < len(spots):
            ahead.append(first_product(*spots[n + 1]))
        green = g_ref[e, 0, 0, k], g_ref[e, 1, 0, k]
        out = product(*ahead[n], *green)
        for p, (whole, change) in enumerate(zip(green, out)):
            whole = whole.astype(jnp.float32) + change * (1.0 / orbitals)
            d_held[e, p, k] = whole.astype(jnp.bfloat16)
        for p in range(parts):
            send(d_held.at[e, p, k], d_ref.at[first + e, p, 0, k], d_sems.at[e, p, k])
    for copy in copies:
        copy.wait()


def dyson(pieces, green, first, kcols, relative, earlier):
    devices, energies, parts, each, rows, orbitals = pieces.shape
    own = green[first : first + energies]
    split = (energies, parts, each, devices, rows, orbitals)
    far_spec = pl.BlockSpec(memory_space=pltpu.HBM)
    return pl.pallas_call(
        functools.partial(dyson_kernel, first, kcols, relative),
        in_specs=[LOCAL, LOCAL] + [far_spec] * len(earlier),
        out_specs=[far_spec, far_spec],
        out_shape=[
            pltpu.HBM((green.shape[0],) + split[1:], jnp.bfloat16),
            pltpu.HBM(green.shape, jnp.bfloat16),
        ],
        input_output_aliases={2 + n: n for n in range(len(earlier))},
        scratch_shapes=[
            pltpu.VMEM(pieces.shape if relative else (1,) * 5 + (orbitals,), jnp.bfloat16),
            pltpu.VMEM(split[:3] + (orbitals, orbitals), jnp.bfloat16),
            pltpu.SemaphoreType.DMA(split[:3]),
            pltpu.SemaphoreType.DMA(split[:3]),
        ],
        cost_estimate=pl.CostEstimate(
            flops=16 * orbitals**3 * each * energies,
            bytes_accessed=16 * pieces.size,
            transcendentals=0,
        ),
        compiler_params=PARAMS,
    )(near(pieces), near(own), *earlier)


def exchange(blocks):
    return lax.all_to_all(blocks, AXES, split_axis=0, concat_axis=0, tiled=True)


def swap(pieces, dims, join=True):
    counts, devices = pieces.counts, math.prod(pieces.counts)
    strides = [math.prod(counts[d + 1 :]) for d in range(len(counts))]

    def level(part, left, offset):
        if not left:
            if offset == 0:
                return part
            pairs = [(d, d ^ offset) for d in range(devices)]
            return lax.ppermute(part, AXES, pairs)
        dim, rest = left[0], left[1:]
        cut = part
        if not isinstance(part, (list, tuple)):
            cut = [lax.slice_in_dim(part, q, q + 1, axis=dim) for q in range(counts[dim])]
        back = [level(c, rest, offset + q * strides[dim]) for q, c in enumerate(cut)]
        if not join:
            return back
        return lax.concatenate(back, dim)

    return Side(counts, level(pieces.blocks, dims, 0))


class Side(typing.NamedTuple):
    counts: tuple
    blocks: typing.Any

    def merged(self):
        return self.blocks.reshape((-1,) + self.blocks.shape[len(self.counts) :])

    @classmethod
    def of(cls, counts, blocks):
        return cls(counts, blocks.reshape(counts + blocks.shape[1:]))


def per_device(green, screened):
    krows, kcols = lax.axis_size("krow"), lax.axis_size("kcol")
    devices = krows * kcols
    energies, parts, _, each, orbitals, width = green.shape
    rows = orbitals // devices
    weights = screened.reshape(screened.shape[:2] + (rows, width))
    blocks = green.reshape(energies, parts, each, devices, rows, width)
    aside = 1 if kcols == 2 and krows in (8, 16) and energies > 1 else 0
    main = energies - aside
    earlier = ()
    if aside:
        counts = (krows // 8, 2, 2, 2, kcols)
        cut = by_offset(blocks, main, aside, kcols, 2 * counts[0])
        cut = [c.reshape((1, 1) + counts[2:] + c.shape[1:]) for c in cut]
        side = Side(counts, [cut[2 * h : 2 * h + 2] for h in range(counts[0])])
        side = swap(side, (0, 1))
        side = swap(side, (3,))
        side = swap(side, (2, 4), join=False)
        turned = fourier(side.blocks, weights, kcols, counts)
        side = swap(Side.of(counts, turned), (4,))
        side = swap(side, (0, 1))
        side = swap(side, (3,))
        side = swap(side, (2,))
        earlier = dyson(side.merged(), green, main, kcols, True, ())
    middle = exchange(by_device(blocks, main))
    middle = fourier(middle, weights, kcols, ())
    middle = exchange(middle)
    sigma, dressed = dyson(middle, green, 0, kcols, False, earlier)
    return sigma.reshape(green.shape), dressed


def solution(mesh):
    spec = P(None, None, "krow", "kcol", None, None)
    return jax.shard_map(
        per_device,
        mesh=mesh,
        in_specs=(spec, P(None, None, AXES)),
        out_specs=(spec, spec),
        check_vma=False,
    )
```
